32 devices in a mesh: grp: 4 (over x, core), dev: 8 (over z, y).
Axes of the slice: x: 2, y: 2, z: 4, core: 2. Of those that a mesh axis runs over, the one named last changes fastest.
Arguments:
- layer_input: bfloat16 [65536, 1024], P(('grp', 'dev')), may hold values from -6 to 6
- hidden_pre: bfloat16 [65536, 1024], P(('grp', 'dev')), may hold values from -6 to 6
- out_grad: bfloat16 [65536, 512], P(('grp', 'dev')), may hold values from -6 to 6
- second_weight: bfloat16 [1024, 512], replicated, may hold values from -0.25 to 0.25
- row_grads: bfloat16 [16384, 128], P(('grp', 'dev')), may hold values from -6 to 6
- row_ids: int32 [16384], P(('grp', 'dev')), may hold values from 0 to 2047
- block_counts: int32 [256], P(('grp', 'dev')), may hold values from 1 to 64, as said below
- emb_table: float32 [16384, 128], P('dev'), may hold values from -4 to 4
- adagrad_state: float32 [16384, 128], P('dev'), may hold values from 0.01 to 1
Outputs:
- grad_first: float32 [1024, 1024], P(('grp', 'dev'))
- grad_second: float32 [1024, 512], P(('grp', 'dev'))
- new_table: float32 [16384, 128], P('dev')
- new_state: float32 [16384, 128], P('dev')
The draws below stay inside these ranges and needn't reach their ends.
Inputs may be any that keep to these rules, and one draw needn't show every extreme that they name: `block_counts`: the used slots of a block are its first ones. In every draw some owner receives full blocks of 64 used slots from every device. `row_ids`: only used slots are read.
All inputs are finite; a program needn't handle non-finite values.
Results may differ from the reference program's by a relative error of at most 0.0029.
Values may be sent and summed in bfloat16 or wider, within the bound.
A program may use at most 128 MiB of HBM per device.

```python
import math
import jax
import jax.numpy as jnp
import numpy as np
from jax import lax

IN = 1024
HID = 1024
OUT = 512
E = 128
TROWS_DEV = 2048
CAP = 64
OWNERS = 8
TOKENS = 65536
BLOCKS = 256
SLOTS = 16384
TABLE_ROWS = 16384


def draw_block_counts(key, part):
    first, second, third = jax.random.split(jax.random.fold_in(key, 11), 3)
    base = jax.random.randint(first, (BLOCKS,), 1, CAP + 1)
    heated = jax.random.randint(second, (OWNERS,), 0, 4) == 0
    forced = jax.random.randint(third, (), 0, OWNERS)
    heated = heated | (jnp.arange(OWNERS) == forced)
    owner = jnp.arange(BLOCKS) % OWNERS
    return jnp.where(heated[owner], CAP, base).astype(jnp.int32)


def place_ends(result, stream_key, least, high):
    place = [jax.random.randint(jax.random.fold_in(stream_key, axis), (), 0, length) for axis, length in enumerate(result.shape)]
    main_axis = result.shape.index(max(result.shape))
    next_to = place[:main_axis] + [(place[main_axis] + 1) % result.shape[main_axis]] + place[main_axis + 1:]
    return result.at[tuple(place)].set(least).at[tuple(next_to)].set(high)


def strengthened(array, own_key, source, target, shards_of, factor):
    def block_of(axis_at):
        return (jnp.arange(array.shape[axis_at]) // (array.shape[axis_at] // shards_of)).reshape((-1,) + (1,) * (array.ndim - 1 - axis_at))

    one_side = jax.random.permutation(own_key, shards_of)[block_of(target)]
    other_side = (block_of(target) + shards_of // 2) % shards_of
    return jnp.where((block_of(source) == one_side) | (block_of(source) == other_side), factor * array, array)


def block_levels(own_key, extent, cuts, least, high):
    loudness, own = 1.0, jax.random.fold_in(own_key, 6)
    for position, parts in cuts:
        steps = jnp.exp(jax.random.uniform(jax.random.fold_in(own, position), (parts,), jnp.float32, least / len(cuts), high / len(cuts)))
        loudness = loudness * jnp.repeat(steps, extent[position] // parts).reshape([-1 if axis == position else 1 for axis in range(len(extent))])
    return loudness


def rank_bounds(amount, skew):
    loads = [(1 << 20) // math.isqrt(standing ** skew) + 1 for standing in range(1, amount + 1)]
    width = 1 + sum(loads) // (1 << 30)
    return np.cumsum(np.array([max(1, weight // width) for weight in loads]))


def ranked_ids(stream_key, extent, amount, skew):
    listing = rank_bounds(amount, skew)
    pick = jax.random.randint(jax.random.fold_in(stream_key, 1), extent, 0, int(listing[amount - 1]))
    rank = jnp.searchsorted(jnp.asarray(listing, jnp.int32), pick, side="right")
    return jax.random.permutation(jax.random.fold_in(stream_key, 2), amount)[rank].astype(jnp.int32)


def centred(key, shape, deviation, bound, cuts=(), held_as=jnp.bfloat16):
    gain = block_levels(key, shape, cuts, -0.22, 0.18) if cuts else 1.0
    values = jax.random.normal(key, shape, jnp.float32) * deviation * gain
    return jnp.minimum(jnp.maximum(values, -bound), bound).astype(held_as)


def noise_with(key, dims, width, reach, pieces, heavy, held_as=jnp.bfloat16):
    drawn = width * jax.random.normal(key, dims, jnp.float32)
    if pieces:
        drawn = drawn * block_levels(key, dims, pieces, -0.22, 0.18)
    return jnp.clip(strengthened(drawn, jax.random.fold_in(key, 3), *heavy), -reach, reach).astype(held_as)


def setup_inputs(seed: int = 0) -> dict:
    streams_of = jax.random.split(jax.random.key(seed), 10)
    return {
        "layer_input": noise_with(streams_of[0], (TOKENS, IN), 1.0, 6.0, ((0, 32),), (0, 1, 32, 2.75)),
        "hidden_pre": noise_with(streams_of[1], (TOKENS, HID), 1.0, 6.0, ((0, 32),), (0, 1, 32, 2.75)),
        "out_grad": centred(streams_of[2], (TOKENS, OUT), 1.0, 6.0, ((0, 32),)),
        "second_weight": centred(streams_of[3], (HID, OUT), OUT ** -0.5, 0.25),
        "row_grads": centred(streams_of[4], (SLOTS, E), 1.0, 6.0, ((0, 32),)),
        "row_ids": place_ends(ranked_ids(streams_of[5], (SLOTS,), TROWS_DEV, 2), jax.random.fold_in(streams_of[5], 3), 0, TROWS_DEV - 1).astype(jnp.int32),
        "block_counts": draw_block_counts(jax.random.fold_in(streams_of[9], 71), 0),
        "emb_table": centred(streams_of[7], (TABLE_ROWS, E), 0.5, 4.0, ((0, 8),), jnp.float32),
        "adagrad_state": jnp.clip(jnp.exp(math.log(1.0) - 4.6051702 * jax.random.uniform(streams_of[8], (TABLE_ROWS, E), jnp.float32) ** block_levels(streams_of[8], (TABLE_ROWS, E), ((0, 8),), -0.2, 0.2)), 0.01, 1.0),
    }


learn_rate = 0.5
epsilon = 1e-08

def reference(layer_input, hidden_pre, out_grad, second_weight, row_grads, row_ids, block_counts, emb_table, adagrad_state):
    active = jnp.maximum(hidden_pre, jnp.zeros_like(hidden_pre))
    back = jnp.dot(out_grad, second_weight.T, preferred_element_type=jnp.float32)
    d_hidden = (back * (hidden_pre > 0).astype(jnp.float32)).astype(jnp.bfloat16)
    contract = (((0,), (0,)), ((), ()))
    grad_first = lax.dot_general(layer_input, d_hidden, contract, preferred_element_type=jnp.float32)
    grad_second = lax.dot_general(active, out_grad, contract, preferred_element_type=jnp.float32)
    slot_index = jnp.arange(row_grads.shape[0], dtype=jnp.int32)
    block_index = slot_index // CAP
    owner = block_index % OWNERS
    usable = slot_index % CAP < block_counts[block_index]
    target = owner * TROWS_DEV + row_ids
    values = row_grads.astype(jnp.float32) * usable.astype(jnp.float32)[:, None]
    table_grad = jax.ops.segment_sum(values, target, num_segments=TABLE_ROWS)
    new_state = adagrad_state + table_grad * table_grad
    new_table = emb_table - learn_rate * table_grad / (jnp.sqrt(new_state) + epsilon)
    return (grad_first, grad_second, new_table, new_state)
```

```python
import functools

import jax
import jax.numpy as jnp
from jax import lax
from jax.experimental import pallas as pl
from jax.experimental.pallas import tpu as pltpu
from jax.sharding import PartitionSpec as P

learn_rate = 0.5
epsilon = 1e-08
MESH = pl.DeviceIdType.MESH
LANES = 128


def kernel(
    G, D,
    x_hbm, h_hbm, og_hbm, w2_hbm, rg_hbm, ids_hbm, tab_hbm, st_hbm,
    g1_ref, g2_ref, ntab_hbm, nst_hbm,
    x_v, h_v, og_v, w2_v, tab_v, st_v, dh_v, lt_v,
    eb, ib,
    cs2, cr2, xs2, xr2, kp2, zs2, zf2, zr2,
    cs1, cr1, xs1, xr1, kp1, zs1, zf1, zr1,
    lsem, cs_s, cr_s, xs_s, xr_s, zs_s, zr_s, e1s, e1r, e2s, e2r,
):
    GX, DH = G // 2, D // 2
    g, d = lax.axis_index("grp"), lax.axis_index("dev")
    gx, c = g // 2, g % 2
    dh, dl = d // 2, d % 2
    tokens = x_v.shape[0]
    R = g1_ref.shape[0]
    DR = D * R
    tile = 256
    f32, bf16 = jnp.float32, jnp.bfloat16

    def local(src, dst, i):
        return pltpu.make_async_copy(src, dst, lsem.at[i])

    loads = [
        local(h_hbm, h_v, 0),
        local(og_hbm, og_v, 1),
        local(w2_hbm, w2_v, 2),
        local(x_hbm, x_v, 3),
        local(rg_hbm.at[d], eb.at[g, d], 4),
        local(ids_hbm.at[d], ib.at[g, d], 5),
        local(tab_hbm, tab_v, 6),
        local(st_hbm, st_v, 7),
    ]
    for load in loads:
        load.start()

    peers = [(gx * 2 + (c + 1) % 2, d)]
    plane = []
    for kx in range(GX):
        for kl in range(2):
            if kx or kl:
                plane.append((kx, kl, ((gx + kx) % GX) * 2 + c, dh * 2 + (dl + kl) % 2))
    line = [(k, ((dh + k) % DH) * 2 + dl) for k in range(1, DH)]
    owners = [(k, (d + k) % D) for k in range(1, D)]
    groups = [(k, (g + k) % G) for k in range(1, G)]
    for kx, kl, pg, pd in plane:
        peers.append((pg, pd))
    for k, pd in owners:
        peers.append((g, pd))
    for k, pg in groups:
        peers.append((pg, d))
    barrier = pltpu.get_barrier_semaphore()
    for peer in peers:
        pl.semaphore_signal(barrier, inc=1, device_id=peer, device_id_type=MESH)
    pl.semaphore_wait(barrier, len(peers))

    def remote(src, dst, ss, rs, to):
        return pltpu.make_async_remote_copy(
            src_ref=src, dst_ref=dst, send_sem=ss, recv_sem=rs, device_id=to, device_id_type=MESH
        )

    pending = []

    def send(*args):
        copy = remote(*args)
        copy.start()
        pending.append(copy)

    for k, pd in owners:
        send(rg_hbm.at[pd], eb.at[g, d], e1s.at[0, k], e1r.at[0, k], (g, pd))
        send(ids_hbm.at[pd], ib.at[g, d], e1s.at[1, k], e1r.at[1, k], (g, pd))

    other = (gx * 2 + (c + 1) % 2, d)

    def transpose(src, target_group, relu):
        cols = pl.ds(pl.multiple_of(target_group * DR, DR), DR)

        def body(t, _):
            rows = pl.ds(pl.multiple_of(t * tile, tile), tile)
            block = src[rows, cols]
            if relu:
                block = jnp.maximum(block, jnp.zeros_like(block))
            lt_v[:, rows] = block.T
            return 0

        lax.fori_loop(0, tokens // tile, body, 0)

    def product(rhs, out_tile):
        width = rhs.shape[1]

        def body(n, _):
            ns = pl.ds(pl.multiple_of(n * tile, tile), tile)
            out_tile(ns, jnp.dot(lt_v[...], rhs[:, ns], preferred_element_type=f32))
            return 0

        lax.fori_loop(0, width // tile, body, 0)

    order = [1 % GX] + [k for k in range(GX) if k != 1 % GX]

    def away(a, src, relu, rhs, cs, cr):
        for kx in order:
            transpose(src, ((gx + kx) % GX) * 2 + (c + 1) % 2, relu)

            def put(ns, value, kx=kx):
                cs[kx, :, ns] = value

            product(rhs, put)
            send(cs.at[kx], cr.at[kx], cs_s.at[a, kx], cr_s.at[a, kx], other)

    def home(a, src, relu, rhs, cr, xs, xr, kp):
        for kx in order:
            transpose(src, ((gx + kx) % GX) * 2 + c, relu)
            remote(cr.at[kx], cr.at[kx], cs_s.at[a, kx], cr_s.at[a, kx], other).wait_recv()

            def put(ns, value, kx=kx):
                value = value + cr[kx, :, ns]
                for b in range(DH):
                    for l in range(2):
                        at = (b * 2 + l) * R
                        piece = value[at : at + R]
                        xs[kx, l, b, :, ns] = piece.astype(bf16)
                        if kx == 0:
                            kp[l, b, :, ns] = piece

            product(rhs, put)
            for px, kl, pg, pd in plane[::-1]:
                if px == kx:
                    i = px * 2 + kl
                    send(xs.at[kx, (dl + kl) % 2], xr.at[i], xs_s.at[a, i], xr_s.at[a, i], (pg, pd))

    def along(a, xr, kp, zs, zf, zr):
        for px, kl, pg, pd in plane:
            i = px * 2 + kl
            remote(xr.at[i], xr.at[i], xs_s.at[a, i], xr_s.at[a, i], (pg, pd)).wait_recv()
        for b in range(DH):
            value = kp[dl, b]
            for px, kl, pg, pd in plane:
                value = value + xr[px * 2 + kl, b].astype(f32)
            zf[b] = value
            zs[b] = value.astype(bf16)
        for k, pd in line[::-1]:
            send(zs.at[(dh + k) % DH], zr.at[k], zs_s.at[a, k], zr_s.at[a, k], (g, pd))

    def finish(a, zf, zr, out):
        value = zf[dh]
        for k, pd in line:
            remote(zr.at[k], zr.at[k], zs_s.at[a, k], zr_s.at[a, k], (g, pd)).wait_recv()
            value = value + zr[k].astype(f32)
        out[...] = value

    loads[0].wait()
    loads[1].wait()
    away(0, h_v, True, og_v, cs2, cr2)
    home(0, h_v, True, og_v, cr2, xs2, xr2, kp2)

    loads[4].wait()
    loads[5].wait()
    for k, pd in owners:
        src = (d + D - k) % D
        remote(eb.at[g, src], eb.at[g, src], e1s.at[0, k], e1r.at[0, k], (g, pd)).wait_recv()
        remote(ib.at[g, src], ib.at[g, src], e1s.at[1, k], e1r.at[1, k], (g, pd)).wait_recv()
    for k, pg in groups:
        send(eb.at[g], eb.at[g], e2s.at[0, k], e2r.at[0, k], (pg, d))
        send(ib.at[g], ib.at[g], e2s.at[1, k], e2r.at[1, k], (pg, d))

    loads[2].wait()

    def back_tile(t, _):
        rows = pl.ds(pl.multiple_of(t * tile, tile), tile)
        back = lax.dot_general(
            og_v[rows, :], w2_v[...], (((1,), (1,)), ((), ())), preferred_element_type=f32
        )
        keep = h_v[rows, :].astype(f32) > 0
        dh_v[rows, :] = jnp.where(keep, back, jnp.zeros_like(back)).astype(bf16)
        return 0

    lax.fori_loop(0, tokens // tile, back_tile, 0)

    loads[3].wait()
    away(1, x_v, False, dh_v, cs1, cr1)
    home(1, x_v, False, dh_v, cr1, xs1, xr1, kp1)
    along(0, xr2, kp2, zs2, zf2, zr2)

    loads[6].wait()
    loads[7].wait()
    for k, pg in groups:
        src = (g + G - k) % G
        remote(eb.at[src], eb.at[src], e2s.at[0, k], e2r.at[0, k], (pg, d)).wait_recv()
        remote(ib.at[src], ib.at[src], e2s.at[1, k], e2r.at[1, k], (pg, d)).wait_recv()
    cap = eb.shape[2]
    pack = LANES // cap
    owned = tab_v.shape[0]

    def owned_tile(t, _):
        start = pl.multiple_of(t * tile, tile)
        rows = pl.ds(start, tile)
        wanted = start + lax.broadcasted_iota(jnp.int32, (tile, LANES), 0)
        total = jnp.zeros((tile, eb.shape[3]), f32)
        for q in range(G):
            parts = []
            for s in range(0, D, pack):
                ids = ib[q, s]
                for e in range(1, pack):
                    ids = jnp.maximum(ids, ib[q, s + e])
                hit = wanted == ids[0:1, :]
                parts.append(jnp.where(hit, 1.0, 0.0).astype(bf16))
            onehot = jnp.concatenate(parts, axis=1)
            total = total + jnp.dot(
                onehot, eb[q].reshape(D * cap, eb.shape[3]), preferred_element_type=f32
            )
        state = st_v[rows, :] + total * total
        st_v[rows, :] = state
        tab_v[rows, :] = tab_v[rows, :] - learn_rate * total / (jnp.sqrt(state) + epsilon)
        return 0

    lax.fori_loop(0, owned // tile, owned_tile, 0)
    stores = [local(tab_v, ntab_hbm, 0), local(st_v, nst_hbm, 1)]
    for store in stores:
        store.start()

    finish(0, zf2, zr2, g2_ref)
    along(1, xr1, kp1, zs1, zf1, zr1)
    finish(1, zf1, zr1, g1_ref)
    for copy in pending:
        copy.wait_send()
    for store in stores:
        store.wait()


def solution(mesh):
    G, D = mesh.shape["grp"], mesh.shape["dev"]

    def on_device(
        layer_input, hidden_pre, out_grad, second_weight,
        row_grads, row_ids, block_counts, emb_table, adagrad_state,
    ):
        T, IN = layer_input.shape
        HID, OUT = second_weight.shape
        E = row_grads.shape[1]
        cap = row_grads.shape[0] // D
        owned = emb_table.shape[0]
        GX, DH = G // 2, D // 2
        pack = LANES // cap
        R1, R2 = IN // (G * D), HID // (G * D)
        lane = jnp.arange(LANES, dtype=jnp.int32)
        mine = lax.axis_index("dev") % pack
        usable = (lane[None, :] % cap < block_counts[:, None]) & (lane[None, :] // cap == mine)
        ids = jnp.where(usable, jnp.tile(row_ids.reshape(D, cap), (1, pack)), -1)
        ids = jnp.broadcast_to(ids[:, None, :], (D, 8, LANES))
        f32, bf16 = jnp.float32, jnp.bfloat16

        def stages(R, N):
            return [
                pltpu.VMEM((GX, D * R, N), f32),
                pltpu.VMEM((GX, D * R, N), f32),
                pltpu.VMEM((GX, 2, DH, R, N), bf16),
                pltpu.VMEM((GX * 2, DH, R, N), bf16),
                pltpu.VMEM((2, DH, R, N), f32),
                pltpu.VMEM((DH, R, N), bf16),
                pltpu.VMEM((DH, R, N), f32),
                pltpu.VMEM((DH, R, N), bf16),
            ]

        hbm = pl.BlockSpec(memory_space=pltpu.HBM)
        vmem = pl.BlockSpec(memory_space=pltpu.VMEM)
        dma = pltpu.SemaphoreType.DMA
        return pl.pallas_call(
            functools.partial(kernel, G, D),
            out_shape=[
                jax.ShapeDtypeStruct((R1, HID), f32),
                jax.ShapeDtypeStruct((R2, OUT), f32),
                jax.ShapeDtypeStruct(emb_table.shape, f32),
                jax.ShapeDtypeStruct(adagrad_state.shape, f32),
            ],
            in_specs=[hbm] * 8,
            out_specs=[vmem, vmem, hbm, hbm],
            scratch_shapes=[
                pltpu.VMEM((T, IN), bf16),
                pltpu.VMEM((T, HID), bf16),
                pltpu.VMEM((T, OUT), bf16),
                pltpu.VMEM((HID, OUT), bf16),
                pltpu.VMEM((owned, E), f32),
                pltpu.VMEM((owned, E), f32),
                pltpu.VMEM((T, HID), bf16),
                pltpu.VMEM((D * R1, T), bf16),
                pltpu.VMEM((G, D, cap, E), bf16),
                pltpu.VMEM((G, D, 8, LANES), jnp.int32),
                *stages(R2, OUT),
                *stages(R1, HID),
                dma((8,)),
                dma((2, GX)), dma((2, GX)),
                dma((2, GX * 2)), dma((2, GX * 2)),
                dma((2, DH)), dma((2, DH)),
                dma((2, D)), dma((2, D)),
                dma((2, G)), dma((2, G)),
            ],
            compiler_params=pltpu.CompilerParams(
                collective_id=0, has_side_effects=True, vmem_limit_bytes=60 * 1024 * 1024
            ),
        )(
            layer_input, hidden_pre, out_grad, second_weight,
            row_grads.reshape(D, cap, E), ids, emb_table, adagrad_state,
        )

    return jax.shard_map(
        on_device,
        mesh=mesh,
        in_specs=(
            P(("grp", "dev"), None),
            P(("grp", "dev"), None),
            P(("grp", "dev"), None),
            P(),
            P(("grp", "dev"), None),
            P(("grp", "dev")),
            P(("grp", "dev")),
            P("dev", None),
            P("dev", None),
        ),
        out_specs=(P(("grp", "dev"), None), P(("grp", "dev"), None), P("dev", None), P("dev", None)),
        check_vma=False,
    )
```

```python
import functools

import jax
import jax.numpy as jnp
from jax import lax
from jax.experimental import pallas as pl
from jax.experimental.pallas import tpu as pltpu
from jax.sharding import PartitionSpec as P

learn_rate = 0.5
epsilon = 1e-08
MESH = pl.DeviceIdType.MESH
LANES = 128


def kernel(
    G, D,
    x_hbm, h_hbm, og_hbm, w2_hbm, rg_hbm, ids_hbm,
    g1_ref, g2_ref, tg_hbm,
    x_v, h_v, og_v, w2_v, wt_v, tg_v, dh_v, lt_v,
    eb, ib,
    cs2, cr2, xs2, xr2, kp2, zs2, zf2, zr2,
    cs1, cr1, xs1, xr1, kp1, zs1, zf1, zr1,
    lsem, cs_s, cr_s, xs_s, xr_s, zs_s, zr_s, e1s, e1r, e2s, e2r,
):
    GX, DH = G // 2, D // 2
    g, d = lax.axis_index("grp"), lax.axis_index("dev")
    gx, c = g // 2, g % 2
    dh, dl = d // 2, d % 2
    tokens = x_v.shape[0]
    R = g1_ref.shape[0]
    DR = D * R
    tile = 256
    wide = min(tokens, 1024)
    f32, bf16 = jnp.float32, jnp.bfloat16

    def local(src, dst, i):
        return pltpu.make_async_copy(src, dst, lsem.at[i])

    loads = [
        local(w2_hbm, w2_v, 0),
        local(h_hbm, h_v, 1),
        local(og_hbm, og_v, 2),
        local(x_hbm, x_v, 3),
        local(rg_hbm.at[d], eb.at[g, d], 4),
        local(ids_hbm.at[d], ib.at[g, d], 5),
    ]
    for load in loads:
        load.start()

    peers = [(gx * 2 + (c + 1) % 2, d)]
    plane = []
    for kx in range(GX):
        for kl in range(2):
            if kx or kl:
                plane.append((kx, kl, ((gx + kx) % GX) * 2 + c, dh * 2 + (dl + kl) % 2))
    line = [(k, ((dh + k) % DH) * 2 + dl) for k in range(1, DH)]
    owners = [(k, (d + k) % D) for k in range(1, D)]
    groups = [(k, (g + k) % G) for k in range(1, G)]
    for kx, kl, pg, pd in plane:
        peers.append((pg, pd))
    for k, pd in owners:
        peers.append((g, pd))
    for k, pg in groups:
        peers.append((pg, d))
    barrier = pltpu.get_barrier_semaphore()
    for peer in peers:
        pl.semaphore_signal(barrier, inc=1, device_id=peer, device_id_type=MESH)
    pl.semaphore_wait(barrier, len(peers))

    def remote(src, dst, ss, rs, to):
        return pltpu.make_async_remote_copy(
            src_ref=src, dst_ref=dst, send_sem=ss, recv_sem=rs, device_id=to, device_id_type=MESH
        )

    pending = []

    def send(*args):
        copy = remote(*args)
        copy.start()
        pending.append(copy)

    for k, pd in owners:
        send(rg_hbm.at[pd], eb.at[g, d], e1s.at[0, k], e1r.at[0, k], (g, pd))
        send(ids_hbm.at[pd], ib.at[g, d], e1s.at[1, k], e1r.at[1, k], (g, pd))

    other = (gx * 2 + (c + 1) % 2, d)

    def transpose(src, target_group, relu):
        cols = pl.ds(pl.multiple_of(target_group * DR, DR), DR)

        for t in range(0, tokens, wide):
            block = src[t : t + wide, cols]
            if relu:
                block = jnp.maximum(block, jnp.zeros_like(block))
            lt_v[:, t : t + wide] = block.T

    def product(rhs, out_tile):
        width = rhs.shape[1]

        def body(n, _):
            ns = pl.ds(pl.multiple_of(n * tile, tile), tile)
            out_tile(ns, jnp.dot(lt_v[...], rhs[:, ns], preferred_element_type=f32))
            return 0

        lax.fori_loop(0, width // tile, body, 0)

    order = [1 % GX] + [k for k in range(GX) if k != 1 % GX]

    def away(only, a, src, relu, rhs, cs, cr):
        for kx in (only,):
            transpose(src, ((gx + kx) % GX) * 2 + (c + 1) % 2, relu)

            def put(ns, value, kx=kx):
                cs[kx, :, ns] = value

            product(rhs, put)
            send(cs.at[kx], cr.at[kx], cs_s.at[a, kx], cr_s.at[a, kx], other)

    def home(only, a, src, relu, rhs, cr, xs, xr, kp):
        for kx in (only,):
            transpose(src, ((gx + kx) % GX) * 2 + c, relu)
            remote(cr.at[kx], cr.at[kx], cs_s.at[a, kx], cr_s.at[a, kx], other).wait_recv()

            def put(ns, value, kx=kx):
                value = value + cr[kx, :, ns]
                for b in range(DH):
                    for l in range(2):
                        at = (b * 2 + l) * R
                        piece = value[at : at + R]
                        xs[kx, l, b, :, ns] = piece.astype(bf16)
                        if kx == 0:
                            kp[l, b, :, ns] = piece

            product(rhs, put)
            for px, kl, pg, pd in plane[::-1]:
                if px == kx:
                    i = px * 2 + kl
                    send(xs.at[kx, (dl + kl) % 2], xr.at[i], xs_s.at[a, i], xr_s.at[a, i], (pg, pd))

    def along(a, xr, kp, zs, zf, zr):
        for px, kl, pg, pd in plane:
            i = px * 2 + kl
            remote(xr.at[i], xr.at[i], xs_s.at[a, i], xr_s.at[a, i], (pg, pd)).wait_recv()
        for b in range(DH):
            value = kp[dl, b]
            for px, kl, pg, pd in plane:
                value = value + xr[px * 2 + kl, b].astype(f32)
            zf[b] = value
            zs[b] = value.astype(bf16)
        for k, pd in line[::-1]:
            send(zs.at[(dh + k) % DH], zr.at[k], zs_s.at[a, k], zr_s.at[a, k], (g, pd))

    def finish(a, zf, zr, out):
        value = zf[dh]
        for k, pd in line:
            remote(zr.at[k], zr.at[k], zs_s.at[a, k], zr_s.at[a, k], (g, pd)).wait_recv()
            value = value + zr[k].astype(f32)
        out[...] = value

    loads[0].wait()
    for n in range(0, w2_v.shape[0], tile):
        wt_v[:, n : n + tile] = w2_v[n : n + tile, :].T
    loads[1].wait()
    loads[2].wait()
    def hand_over():
        loads[4].wait()
        loads[5].wait()
        for k, pd in owners:
            src = (d + D - k) % D
            remote(eb.at[g, src], eb.at[g, src], e1s.at[0, k], e1r.at[0, k], (g, pd)).wait_recv()
            remote(ib.at[g, src], ib.at[g, src], e1s.at[1, k], e1r.at[1, k], (g, pd)).wait_recv()
        for k, pg in groups:
            send(eb.at[g], eb.at[g], e2s.at[0, k], e2r.at[0, k], (pg, d))
            send(ib.at[g], ib.at[g], e2s.at[1, k], e2r.at[1, k], (pg, d))

    for only in order:
        away(only, 0, h_v, True, og_v, cs2, cr2)
    for only in order:
        home(only, 0, h_v, True, og_v, cr2, xs2, xr2, kp2)
    hand_over()

    def back_tile(t, _):
        rows = pl.ds(pl.multiple_of(t * tile, tile), tile)
        back = jnp.dot(og_v[rows, :], wt_v[...], preferred_element_type=f32)
        keep = h_v[rows, :].astype(f32) > 0
        dh_v[rows, :] = jnp.where(keep, back, jnp.zeros_like(back)).astype(bf16)
        return 0

    lax.fori_loop(0, tokens // tile, back_tile, 0)

    loads[3].wait()
    for only in order:
        away(only, 1, x_v, False, dh_v, cs1, cr1)
    for only in order:
        home(only, 1, x_v, False, dh_v, cr1, xs1, xr1, kp1)
    along(0, xr2, kp2, zs2, zf2, zr2)

    for k, pg in groups:
        src = (g + G - k) % G
        remote(eb.at[src], eb.at[src], e2s.at[0, k], e2r.at[0, k], (pg, d)).wait_recv()
        remote(ib.at[src], ib.at[src], e2s.at[1, k], e2r.at[1, k], (pg, d)).wait_recv()
    cap = eb.shape[2]
    pack = LANES // cap
    owned = tg_v.shape[0]

    def owned_tile(t, _):
        start = pl.multiple_of(t * tile, tile)
        rows = pl.ds(start, tile)
        wanted = start + lax.broadcasted_iota(jnp.int32, (tile, LANES), 0)
        total = jnp.zeros((tile, eb.shape[3]), f32)
        for q in range(G):
            parts = []
            for s in range(0, D, pack):
                ids = ib[q, s]
                for e in range(1, pack):
                    ids = jnp.maximum(ids, ib[q, s + e])
                hit = wanted == ids[0:1, :]
                parts.append(jnp.where(hit, 1.0, 0.0).astype(bf16))
            onehot = jnp.concatenate(parts, axis=1)
            total = total + jnp.dot(
                onehot, eb[q].reshape(D * cap, eb.shape[3]), preferred_element_type=f32
            )
        tg_v[rows, :] = total
        return 0

    lax.fori_loop(0, owned // tile, owned_tile, 0)
    stores = [local(tg_v, tg_hbm, 0)]
    for store in stores:
        store.start()

    along(1, xr1, kp1, zs1, zf1, zr1)
    finish(0, zf2, zr2, g2_ref)
    finish(1, zf1, zr1, g1_ref)
    for copy in pending:
        copy.wait_send()
    for store in stores:
        store.wait()


def update(g1_in, g2_in, sum_in, tab_in, st_in, g1_out, g2_out, tab_out, st_out):
    g1_out[...] = g1_in[...]
    g2_out[...] = g2_in[...]
    total = sum_in[...]
    state = st_in[...] + total * total
    st_out[...] = state
    tab_out[...] = tab_in[...] - learn_rate * total / (jnp.sqrt(state) + epsilon)


def solution(mesh):
    G, D = mesh.shape["grp"], mesh.shape["dev"]

    def on_device(
        layer_input, hidden_pre, out_grad, second_weight,
        row_grads, row_ids, block_counts, emb_table, adagrad_state,
    ):
        T, IN = layer_input.shape
        HID, OUT = second_weight.shape
        E = row_grads.shape[1]
        cap = row_grads.shape[0] // D
        owned = emb_table.shape[0]
        GX, DH = G // 2, D // 2
        pack = LANES // cap
        R1, R2 = IN // (G * D), HID // (G * D)
        lane = jnp.arange(LANES, dtype=jnp.int32)
        mine = lax.axis_index("dev") % pack
        usable = (lane[None, :] % cap < block_counts[:, None]) & (lane[None, :] // cap == mine)
        ids = jnp.where(usable, jnp.tile(row_ids.reshape(D, cap), (1, pack)), -1)
        ids = ids[:, None, :]
        f32, bf16 = jnp.float32, jnp.bfloat16

        def stages(R, N):
            return [
                pltpu.VMEM((GX, D * R, N), f32),
                pltpu.VMEM((GX, D * R, N), f32),
                pltpu.VMEM((GX, 2, DH, R, N), bf16),
                pltpu.VMEM((GX * 2, DH, R, N), bf16),
                pltpu.VMEM((2, DH, R, N), f32),
                pltpu.VMEM((DH, R, N), bf16),
                pltpu.VMEM((DH, R, N), f32),
                pltpu.VMEM((DH, R, N), bf16),
            ]

        hbm = pl.BlockSpec(memory_space=pltpu.HBM)
        vmem = pl.BlockSpec(memory_space=pltpu.VMEM)
        dma = pltpu.SemaphoreType.DMA
        g1, g2, summed = pl.pallas_call(
            functools.partial(kernel, G, D),
            out_shape=[
                jax.ShapeDtypeStruct((R1, HID), f32),
                jax.ShapeDtypeStruct((R2, OUT), f32),
                jax.ShapeDtypeStruct(emb_table.shape, f32),
            ],
            in_specs=[hbm] * 6,
            out_specs=[vmem, vmem, hbm],
            scratch_shapes=[
                pltpu.VMEM((T, IN), bf16),
                pltpu.VMEM((T, HID), bf16),
                pltpu.VMEM((T, OUT), bf16),
                pltpu.VMEM((HID, OUT), bf16),
                pltpu.VMEM((OUT, HID), bf16),
                pltpu.VMEM((owned, E), f32),
                pltpu.VMEM((T, HID), bf16),
                pltpu.VMEM((D * R1, T), bf16),
                pltpu.VMEM((G, D, cap, E), bf16),
                pltpu.VMEM((G, D, 1, LANES), jnp.int32),
                *stages(R2, OUT),
                *stages(R1, HID),
                dma((8,)),
                dma((2, GX)), dma((2, GX)),
                dma((2, GX * 2)), dma((2, GX * 2)),
                dma((2, DH)), dma((2, DH)),
                dma((2, D)), dma((2, D)),
                dma((2, G)), dma((2, G)),
            ],
            compiler_params=pltpu.CompilerParams(
                collective_id=0, has_side_effects=True, vmem_limit_bytes=60 * 1024 * 1024
            ),
        )(
            layer_input, hidden_pre, out_grad, second_weight,
            row_grads.reshape(D, cap, E), ids,
        )
        steps = 4
        rows = pl.BlockSpec((owned // steps, E), lambda i: (i, 0))
        part1 = pl.BlockSpec((R1, HID // steps), lambda i: (0, i))
        part2 = pl.BlockSpec((R2, OUT // steps), lambda i: (0, i))
        return pl.pallas_call(
            update,
            grid=(steps,),
            out_shape=[
                jax.ShapeDtypeStruct((R1, HID), f32),
                jax.ShapeDtypeStruct((R2, OUT), f32),
                jax.ShapeDtypeStruct(emb_table.shape, f32),
                jax.ShapeDtypeStruct(adagrad_state.shape, f32),
            ],
            in_specs=[part1, part2, rows, rows, rows],
            out_specs=[part1, part2, rows, rows],
        )(g1, g2, summed, emb_table, adagrad_state)

    return jax.shard_map(
        on_device,
        mesh=mesh,
        in_specs=(
            P(("grp", "dev"), None),
            P(("grp", "dev"), None),
            P(("grp", "dev"), None),
            P(),
            P(("grp", "dev"), None),
            P(("grp", "dev")),
            P(("grp", "dev")),
            P("dev", None),
            P("dev", None),
        ),
        out_specs=(P(("grp", "dev"), None), P(("grp", "dev"), None), P("dev", None), P("dev", None)),
        check_vma=False,
    )
```
